32 devices in a mesh: grp: 8 (over z, x), dom: 4 (over y, core).
Axes of the slice: x: 2, y: 2, z: 4, core: 2. Of those that a mesh axis runs over, the one named last changes fastest.
Arguments:
- positions: float32 [3, 4096, 512], P(None, ('grp', 'dom')), may hold values from 0 to 1
- velocities: float32 [3, 4096, 512], P(None, ('grp', 'dom')), may hold values from -6 to 6
- masses: float32 [4096, 512], P(('grp', 'dom')), may hold values from 0.5 to 2
- block_halo: int32 [4096], P(('grp', 'dom')), may hold values from 0 to 4095, as said below
- block_shift: int32 [3, 4096], P(None, ('grp', 'dom')), may hold values from -1 to 1
- block_live: int32 [4096], P(('grp', 'dom')), may hold values from 64 to 512
- block_count: int32 [32], P(('grp', 'dom')), may hold values from 32 to 128
- home_slot: int32 [4096], replicated, may hold values from 0 to 4095, as said below
Outputs:
- halo_table: float32 [11, 4096], P(None, ('grp', 'dom'))
- kinetic: float32 [4096, 512], P(('grp', 'dom'))
- radial: float32 [4096, 512], P(('grp', 'dom'))
The draws below stay inside these ranges and needn't reach their ends.
Inputs may be any that keep to these rules, and one draw needn't show every extreme that they name: A permutation: the halo h is owned by the device of index home_slot[h] // 128 (grp+dom order), in its column home_slot[h] % 128. `block_halo`: the owner of a block's halo lies in the block's own index of grp or in the next one (index + 1, wrapping around); both occur.
All inputs are finite; a program needn't handle non-finite values.
Results may differ from the reference program's by a relative error of at most 0.0003.
Values sent between devices are 32-bit elements; how exact they have to be, the bound alone decides.
A program may use at most 64 MiB of HBM per device.

```python
import math
import jax
import jax.numpy as jnp
from jax import lax

BS = 512
BLK_DEV = 128
HALO_DEV = 128
NB = 4096
HALOS = 4096
N_GRP = 8
N_DOM = 4
DEVICES = 32


def owner_table(key):
    return jax.random.permutation(jax.random.fold_in(key, 11), HALOS).astype(jnp.int32)


def draw_home_slot(key, part):
    return owner_table(key)


def draw_block_halo(key, part):
    home = owner_table(key)
    inverse = jnp.argsort(home).astype(jnp.int32)
    window = N_DOM * HALO_DEV
    first_key, second_key, third_key = jax.random.split(jax.random.fold_in(key, 23), 3)
    limit = jax.random.randint(first_key, (NB,), 1, 2 * window + 1)
    picked = jax.random.randint(second_key, (NB,), 0, limit)
    mixing = jax.random.permutation(third_key, 2 * window).astype(jnp.int32)
    picked = mixing[picked]
    group_index = jnp.arange(NB, dtype=jnp.int32) // BLK_DEV // N_DOM
    column = (group_index + picked // window) % N_GRP * window + picked % window
    return inverse[column].astype(jnp.int32)


def touch_ends(values, rng, least, top_value):
    extent = values.shape
    spot = [jax.random.randint(jax.random.fold_in(rng, axis), (), 0, extent[axis]) for axis in range(len(extent))]
    values = values.at[tuple(spot)].set(least)
    longest = extent.index(max(extent))
    spot[longest] = (spot[longest] + 1) % extent[longest]
    return values.at[tuple(spot)].set(top_value)


def steps_of(rng, dims, cuts, smallest, top_value):
    level = 1.0
    for axis_at, shards_of in cuts:
        draws = jax.random.uniform(jax.random.fold_in(jax.random.fold_in(rng, 6), axis_at), (shards_of,), jnp.float32, smallest / len(cuts), top_value / len(cuts))
        level = level * jnp.repeat(jnp.exp(draws), dims[axis_at] // shards_of).reshape((-1,) + (1,) * (len(dims) - 1 - axis_at))
    return level


def normal_values(own_key, extent, scale, bound, pieces=(), kind=jnp.bfloat16):
    entries = scale * jax.random.normal(own_key, extent, jnp.float32)
    if pieces:
        entries = entries * steps_of(own_key, extent, pieces, -0.22, 0.18)
    return jnp.clip(entries, -bound, bound).astype(kind)


def setup_inputs(seed: int = 0) -> dict:
    key_of = jax.random.split(jax.random.key(seed), 9)
    positions = jnp.clip(1.0 * jax.random.uniform(key_of[0], (3, NB, BS), jnp.float32) ** steps_of(key_of[0], (3, NB, BS), ((1, 32),), -0.2, 0.2), 0.0, 1.0)
    velocities = normal_values(key_of[1], (3, NB, BS), 1.0, 6.0, ((1, 32),), jnp.float32)
    masses = jnp.clip(jnp.exp(math.log(2.0) - 1.3862944 * jax.random.uniform(key_of[2], (NB, BS), jnp.float32) ** steps_of(key_of[2], (NB, BS), ((0, 32),), -0.2, 0.2)), 0.5, 2.0)
    block_halo = draw_block_halo(jax.random.fold_in(key_of[8], 71), 0)
    block_shift = touch_ends(jax.random.randint(key_of[4], (3, NB), -1, 2), jax.random.fold_in(key_of[4], 1), -1, 1).astype(jnp.int32)
    block_live = touch_ends(jax.random.randint(key_of[5], (NB,), BS // 8, BS + 1), jax.random.fold_in(key_of[5], 1), BS // 8, BS).astype(jnp.int32)
    block_count = touch_ends(jax.random.randint(key_of[6], (DEVICES,), max(1, BLK_DEV // 4), BLK_DEV + 1), jax.random.fold_in(key_of[6], 1), max(1, BLK_DEV // 4), BLK_DEV).astype(jnp.int32)
    home_slot = draw_home_slot(jax.random.fold_in(key_of[8], 71), 0)
    return {"positions": positions, "velocities": velocities, "masses": masses, "block_halo": block_halo, "block_shift": block_shift, "block_live": block_live, "block_count": block_count, "home_slot": home_slot}


BOX = 1.0
EPSILON = 1e-6


def crossed(first, second):
    return jnp.stack([first[1] * second[2] - first[2] * second[1],
                      first[2] * second[0] - first[0] * second[2],
                      first[0] * second[1] - first[1] * second[0]])


def block_moments(positions, velocities, masses, block_shift, block_live, valid):
    lanes = jnp.arange(masses.shape[1], dtype=jnp.int32)
    live_mask = ((lanes[None, :] < block_live[:, None]) & valid[:, None]).astype(masses.dtype)
    weights = masses * live_mask
    unwrapped = positions + BOX * block_shift.astype(positions.dtype)[:, :, None]
    speed_sq = jnp.sum(velocities * velocities, axis=0)
    angular = crossed(unwrapped, velocities)
    rows = [jnp.sum(weights, axis=1)[None], jnp.sum(weights * unwrapped, axis=2),
            jnp.sum(weights * velocities, axis=2), jnp.sum(weights * speed_sq, axis=1)[None],
            jnp.sum(weights * angular, axis=2)]
    return jnp.concatenate(rows, axis=0), live_mask, unwrapped


def halo_properties(sums, total, halos):
    heavy = jnp.maximum(sums[0], 1.0)
    centre = sums[1:4] / heavy
    drift = sums[4:7] / heavy
    spread = sums[7] / heavy - jnp.sum(drift * drift, axis=0)
    spin = sums[8:11] / heavy - crossed(centre, drift)
    share = sums[0] * halos / total
    return jnp.concatenate([share[None], centre, drift, spread[None], spin], axis=0)


def particle_outputs(unwrapped, velocities, live_mask, stats):
    centre = stats[0:3][:, :, None]
    drift = stats[3:6][:, :, None]
    spread = stats[6][:, None]
    offset = velocities - drift
    kinetic = jnp.sum(offset * offset, axis=0) / (3.0 * spread + EPSILON)
    distance = unwrapped - centre
    radial = jnp.sum(distance * distance, axis=0)
    return kinetic * live_mask, radial * live_mask


def reference(positions, velocities, masses, block_halo, block_shift, block_live, block_count, home_slot):
    groups = block_count.shape[0]
    total_blocks = masses.shape[0]
    width = masses.shape[1]
    grouped_pos = positions.reshape(3, groups, BLK_DEV, width).transpose(1, 0, 2, 3)
    grouped_vel = velocities.reshape(3, groups, BLK_DEV, width).transpose(1, 0, 2, 3)
    grouped_mass = masses.reshape(groups, BLK_DEV, width)
    grouped_shift = block_shift.reshape(3, groups, BLK_DEV).transpose(1, 0, 2)
    grouped_live = block_live.reshape(groups, BLK_DEV)
    valid = jnp.arange(BLK_DEV, dtype=jnp.int32)[None, :] < block_count[:, None]

    def per_group(items):
        place, speed, weight, shift, alive, usable = items
        return block_moments(place, speed, weight, shift, alive, usable)[0]

    moments = lax.map(per_group, (grouped_pos, grouped_vel, grouped_mass, grouped_shift, grouped_live, valid))
    moments = moments.transpose(1, 0, 2).reshape(11, total_blocks)
    slots = home_slot[block_halo]
    halos = home_slot.shape[0]
    sums = jnp.zeros((11, halos), moments.dtype).at[:, slots].add(moments)
    total = jnp.sum(moments[0])
    halo_table = halo_properties(sums, total, halos)
    stats = halo_table[1:8][:, slots].reshape(7, groups, BLK_DEV).transpose(1, 0, 2)

    def outputs(items):
        place, speed, weight, shift, alive, usable, local_stats = items
        _, live_mask, unwrapped = block_moments(place, speed, weight, shift, alive, usable)
        return particle_outputs(unwrapped, speed, live_mask, local_stats)

    kinetic, radial = lax.map(outputs, (grouped_pos, grouped_vel, grouped_mass, grouped_shift, grouped_live, valid, stats))
    return halo_table, kinetic.reshape(total_blocks, width), radial.reshape(total_blocks, width)
```

```python
import functools

import jax
import jax.numpy as jnp
from jax import lax
from jax.experimental import pallas as pl
from jax.experimental.pallas import tpu as pltpu
from jax.sharding import PartitionSpec as P

BOX = 1.0
EPSILON = 1e-06
MESH = pl.DeviceIdType.MESH
F32 = jnp.float32
BF16 = jnp.bfloat16
LANES = 128
CHUNKS = 4
MASS_ROW = 11


def pieces(x):
    hi = x.astype(BF16).astype(F32)
    rest = x - hi
    mid = rest.astype(BF16).astype(F32)
    return hi, mid, rest - mid


def quotient(x, n):
    return x >> (n.bit_length() - 1) if n & (n - 1) == 0 else x // n


def crossed(a, b):
    return (a[1] * b[2] - a[2] * b[1], a[2] * b[0] - a[0] * b[2], a[0] * b[1] - a[1] * b[0])


def kernel(
    groups, domains, owned, halos,
    pos_hbm, vel_hbm, mass_hbm, halo_ref, shift_ref, live_ref, count_ref, home_ref,
    table_ref, kin_hbm, rad_hbm,
    pos, vel, mass, kin, rad, cols, moments, tables, sums_in, stats, total_out, totals_in,
    in_sem, out_sem, send1, recv1, send2, recv2, send3, recv3,
):
    blocks, width = mass.shape
    rows = blocks // CHUNKS
    slots_n = 2 * domains
    g = lax.axis_index("grp")
    d = lax.axis_index("dom")

    def peer(dg, dd):
        return {"grp": lax.rem(g + dg % groups, groups), "dom": lax.rem(d + dd % domains, domains)}

    loads = []
    for c in range(CHUNKS):
        part = pl.ds(c * rows, rows)
        group = [
            pltpu.make_async_copy(mass_hbm.at[part], mass.at[part], in_sem.at[3 * c]),
            pltpu.make_async_copy(pos_hbm.at[:, part], pos.at[:, part], in_sem.at[3 * c + 1]),
            pltpu.make_async_copy(vel_hbm.at[:, part], vel.at[:, part], in_sem.at[3 * c + 2]),
        ]
        for copy in group:
            copy.start()
        loads.append(group)

    partners = {(0, dd) for dd in range(domains)}
    partners |= {(1 % groups, dd) for dd in range(domains)}
    partners |= {(-1 % groups, dd) for dd in range(domains)}
    partners |= {(dg, 0) for dg in range(groups)}
    partners = sorted(partners - {(0, 0)})
    barrier = pltpu.get_barrier_semaphore()
    for dg, dd in partners:
        pl.semaphore_signal(barrier, inc=1, device_id=peer(dg, dd), device_id_type=MESH)

    lane = lax.broadcasted_iota(jnp.int32, (blocks, LANES), 1)
    row = lax.broadcasted_iota(jnp.int32, (blocks, 1), 0)
    packed = jnp.concatenate(
        [
            halo_ref[...].astype(F32),
            live_ref[...].astype(F32),
            shift_ref[...].astype(F32) * BOX,
            jnp.zeros((LANES - 5, blocks), F32),
        ],
        axis=0,
    )
    turned = packed.T
    live_col = jnp.where(row < count_ref[0], turned[:, 1:2], 0.0)
    cols[...] = jnp.where(lane == 1, live_col, turned)

    halo = turned[:, 0:1].astype(jnp.int32)
    home = home_ref[...]
    home_rows = home.shape[0]
    row_pick = lax.broadcasted_iota(jnp.int32, (blocks, home_rows), 1) == quotient(halo, LANES)
    split = jnp.concatenate([(home >> 8).astype(F32), (home & 255).astype(F32)], axis=1)
    picked = jnp.dot(
        row_pick.astype(F32).astype(BF16), split.astype(BF16), preferred_element_type=F32
    )
    value = picked[:, :LANES] * 256.0 + picked[:, LANES:]
    slot = jnp.sum(jnp.where(lane == (halo & (LANES - 1)), value, 0.0), axis=1, keepdims=True)
    slot = slot.astype(jnp.int32)
    owner = quotient(slot, owned)
    owner_grp = quotient(owner, domains)
    turn = owner - owner_grp * domains - d
    turn = jnp.where(turn < 0, turn + domains, turn)
    column = (jnp.where(owner_grp == g, 0, domains) + turn) * owned + slot - owner * owned
    spread_lanes = lax.broadcasted_iota(jnp.int32, (blocks, slots_n * owned), 1)
    onehot = (spread_lanes == column).astype(F32).astype(BF16)

    lane8 = lax.broadcasted_iota(jnp.int32, (8, LANES), 1)
    position8 = lax.broadcasted_iota(jnp.int32, (8, width), 1).astype(F32)

    def fold(x):
        parts = [x[:, i * LANES:(i + 1) * LANES] for i in range(width // LANES)]
        return jnp.sum(functools.reduce(lambda a, b: a + b, parts), axis=1, keepdims=True)

    def moment_rows(start):
        at = pl.ds(start, 8)
        col = cols[at]
        w = jnp.where(position8 < col[:, 1:2], mass[at], 0.0)
        u = [pos[k, at] + col[:, 2 + k:3 + k] for k in range(3)]
        v = [vel[k, at] for k in range(3)]
        wv = [w * x for x in v]
        made = [w] + [w * x for x in u] + wv
        made += [wv[0] * v[0] + wv[1] * v[1] + wv[2] * v[2]]
        made += list(crossed(u, wv))
        out = jnp.zeros((8, LANES), F32)
        for k, x in enumerate(made):
            out = jnp.where(lane8 == k, fold(x), out)
        moments[at] = out

    for c in range(CHUNKS):
        for copy in loads[c]:
            copy.wait()

        def step(i, carry, c=c):
            moment_rows(pl.multiple_of(c * rows + i * 8, 8))
            return carry

        lax.fori_loop(0, rows // 8, step, 0, unroll=True)

    by_row = moments[...].T[:16]
    mass_sum = jnp.sum(by_row[0:1], axis=1, keepdims=True)
    stacked = jnp.concatenate(pieces(by_row), axis=0).astype(BF16)
    product = jnp.dot(stacked, onehot, preferred_element_type=F32)
    product = product[:16] + product[16:32] + product[32:48]
    row16 = lax.broadcasted_iota(jnp.int32, (16, owned), 0)
    for k in range(slots_n):
        tables[k] = jnp.where(row16 == MASS_ROW, mass_sum, product[:, k * owned:(k + 1) * owned])

    pl.semaphore_wait(barrier, len(partners))

    order = sorted(range(1, slots_n), key=lambda k: -k)
    first = {}
    for k in order:
        dg, dd = divmod(k, domains)
        first[k] = pltpu.make_async_remote_copy(
            src_ref=tables.at[k], dst_ref=sums_in.at[k],
            send_sem=send1.at[k], recv_sem=recv1.at[k],
            device_id=peer(dg, dd), device_id_type=MESH,
        )
        first[k].start()

    sums = tables[0]
    for k in range(1, domains):
        first[k].wait_recv()
        sums = sums + sums_in[k]
    group_total = sums[MASS_ROW:MASS_ROW + 1]
    total_out[0] = group_total
    for k in range(domains, slots_n):
        first[k].wait_recv()
        sums = sums + sums_in[k]

    heavy_inv = 1.0 / jnp.maximum(sums[0:1], 1.0)
    scaled = sums[1:11] * heavy_inv
    centre = [scaled[k:k + 1] for k in range(3)]
    drift = [scaled[3 + k:4 + k] for k in range(3)]
    spread = scaled[6:7] - (drift[0] * drift[0] + drift[1] * drift[1] + drift[2] * drift[2])
    stats[0] = jnp.concatenate(
        centre + drift + [spread, 1.0 / (3.0 * spread + EPSILON)], axis=0
    )
    turned_spin = crossed(centre, drift)
    spin = [scaled[7 + k:8 + k] - turned_spin[k] for k in range(3)]

    second = {}
    for k in order:
        dg, dd = divmod(k, domains)
        second[k] = pltpu.make_async_remote_copy(
            src_ref=stats.at[0], dst_ref=stats.at[k],
            send_sem=send2.at[k], recv_sem=recv2.at[k],
            device_id=peer(-dg, -dd), device_id_type=MESH,
        )
        second[k].start()
    third = {}
    for dg in range(1, groups):
        third[dg] = pltpu.make_async_remote_copy(
            src_ref=total_out.at[0], dst_ref=totals_in.at[dg],
            send_sem=send3.at[dg], recv_sem=recv3.at[dg],
            device_id=peer(dg, 0), device_id_type=MESH,
        )
        third[dg].start()

    for k in range(1, slots_n):
        second[k].wait_recv()
    every = jnp.concatenate([stats[k] for k in range(slots_n)], axis=1)
    gathered = jnp.zeros((blocks, 8), F32)
    for piece in pieces(every):
        gathered = gathered + lax.dot_general(
            onehot, piece.astype(BF16), (((1,), (1,)), ((), ())), preferred_element_type=F32
        )
    moments[:, 0:8] = gathered

    def output_rows(start):
        at = pl.ds(start, 8)
        col = cols[at]
        mean = moments[at]
        live = position8 < col[:, 1:2]
        kinetic = 0.0
        radial = 0.0
        for k in range(3):
            distance = (pos[k, at] + col[:, 2 + k:3 + k]) - mean[:, k:k + 1]
            radial = radial + distance * distance
            offset = vel[k, at] - mean[:, 3 + k:4 + k]
            kinetic = kinetic + offset * offset
        kin[at] = jnp.where(live, kinetic * mean[:, 7:8], 0.0)
        rad[at] = jnp.where(live, radial, 0.0)

    stores = []
    for c in range(CHUNKS):

        def step(i, carry, c=c):
            output_rows(pl.multiple_of(c * rows + i * 8, 8))
            return carry

        lax.fori_loop(0, rows // 8, step, 0, unroll=True)
        part = pl.ds(c * rows, rows)
        group = [
            pltpu.make_async_copy(kin.at[part], kin_hbm.at[part], out_sem.at[2 * c]),
            pltpu.make_async_copy(rad.at[part], rad_hbm.at[part], out_sem.at[2 * c + 1]),
        ]
        for copy in group:
            copy.start()
        stores += group

    total = group_total
    for dg in range(1, groups):
        third[dg].wait_recv()
        total = total + totals_in[dg]
    share = sums[0:1] * float(halos) / total
    table_ref[...] = jnp.concatenate([share] + centre + drift + [spread] + spin, axis=0)

    for k in order:
        first[k].wait_send()
        second[k].wait_send()
    for dg in range(1, groups):
        third[dg].wait_send()
    for copy in stores:
        copy.wait()


def solution(mesh):
    groups, domains = mesh.shape["grp"], mesh.shape["dom"]

    def local(
        positions, velocities, masses, block_halo, block_shift, block_live, block_count, home_slot
    ):
        blocks, width = masses.shape
        halos = home_slot.shape[0]
        owned = halos // (groups * domains)
        slots_n = 2 * domains
        vmem = pl.BlockSpec(memory_space=pltpu.VMEM)
        smem = pl.BlockSpec(memory_space=pltpu.SMEM)
        hbm = pl.BlockSpec(memory_space=pl.ANY)
        dma = pltpu.SemaphoreType.DMA
        return pl.pallas_call(
            functools.partial(kernel, groups, domains, owned, halos),
            out_shape=(
                jax.ShapeDtypeStruct((11, owned), F32),
                jax.ShapeDtypeStruct((blocks, width), F32),
                jax.ShapeDtypeStruct((blocks, width), F32),
            ),
            in_specs=[hbm, hbm, hbm, vmem, vmem, vmem, smem, vmem],
            out_specs=(vmem, hbm, hbm),
            scratch_shapes=[
                pltpu.VMEM((3, blocks, width), F32),
                pltpu.VMEM((3, blocks, width), F32),
                pltpu.VMEM((blocks, width), F32),
                pltpu.VMEM((blocks, width), F32),
                pltpu.VMEM((blocks, width), F32),
                pltpu.VMEM((blocks, LANES), F32),
                pltpu.VMEM((blocks, LANES), F32),
                pltpu.VMEM((slots_n, 16, owned), F32),
                pltpu.VMEM((slots_n, 16, owned), F32),
                pltpu.VMEM((slots_n, 8, owned), F32),
                pltpu.VMEM((1, 1, owned), F32),
                pltpu.VMEM((groups, 1, owned), F32),
                dma((3 * CHUNKS,)),
                dma((2 * CHUNKS,)),
                dma((slots_n,)),
                dma((slots_n,)),
                dma((slots_n,)),
                dma((slots_n,)),
                dma((groups,)),
                dma((groups,)),
            ],
            compiler_params=pltpu.CompilerParams(collective_id=0, has_side_effects=True),
        )(
            positions, velocities, masses,
            block_halo.reshape(1, blocks), block_shift, block_live.reshape(1, blocks),
            block_count, home_slot.reshape(halos // LANES, LANES),
        )

    return jax.shard_map(
        local,
        mesh=mesh,
        in_specs=(
            P(None, ("grp", "dom"), None),
            P(None, ("grp", "dom"), None),
            P(("grp", "dom"), None),
            P(("grp", "dom")),
            P(None, ("grp", "dom")),
            P(("grp", "dom")),
            P(("grp", "dom")),
            P(),
        ),
        out_specs=(P(None, ("grp", "dom")), P(("grp", "dom"), None), P(("grp", "dom"), None)),
        check_vma=False,
    )
```

```python
import functools

import jax
import jax.numpy as jnp
from jax import lax
from jax.experimental import pallas as pl
from jax.experimental.pallas import tpu as pltpu
from jax.sharding import PartitionSpec as P

BOX = 1.0
EPSILON = 1e-06
MESH = pl.DeviceIdType.MESH
F32 = jnp.float32
BF16 = jnp.bfloat16
LANES = 128
CHUNKS = 4
MASS_ROW = 11


def pieces(x):
    hi = x.astype(BF16).astype(F32)
    rest = x - hi
    mid = rest.astype(BF16).astype(F32)
    return hi, mid, rest - mid


def quotient(x, n):
    return x >> (n.bit_length() - 1) if n & (n - 1) == 0 else x // n


def crossed(a, b):
    return (a[1] * b[2] - a[2] * b[1], a[2] * b[0] - a[0] * b[2], a[0] * b[1] - a[1] * b[0])


def exchange_kernel(
    groups, domains, owned,
    pos_hbm, vel_hbm, mass_hbm, halo_ref, shift_ref, live_ref, count_ref, home_ref,
    pos, vel, means_ref, sums_ref,
    mass, cols, moments, tables, parts_in, own, near_in, ahead_in, behind_in, rest_in, totals_in,
    in_sem, send1, recv1, send_near, recv_near, send_up, recv_up, send_down, recv_down,
    send_rest, recv_rest, send_total, recv_total,
):
    blocks, width = mass.shape
    rows = blocks // CHUNKS
    g = lax.axis_index("grp")
    d = lax.axis_index("dom")

    def peer(dg, dd):
        return {"grp": lax.rem(g + dg % groups, groups), "dom": lax.rem(d + dd % domains, domains)}

    def remote(src, dst, send, recv, dg, dd):
        return pltpu.make_async_remote_copy(
            src_ref=src, dst_ref=dst, send_sem=send, recv_sem=recv,
            device_id=peer(dg, dd), device_id_type=MESH,
        )

    partners = {(0, dd) for dd in range(domains)}
    partners |= {(1 % groups, dd) for dd in range(domains)}
    partners |= {(-1 % groups, dd) for dd in range(domains)}
    partners |= {(dg, 0) for dg in range(groups)}
    partners = sorted(partners - {(0, 0)})
    barrier = pltpu.get_barrier_semaphore()
    for dg, dd in partners:
        pl.semaphore_signal(barrier, inc=1, device_id=peer(dg, dd), device_id_type=MESH)

    loads = []
    for c in range(CHUNKS):
        part = pl.ds(c * rows, rows)
        group = [
            pltpu.make_async_copy(mass_hbm.at[part], mass.at[part], in_sem.at[3 * c]),
            pltpu.make_async_copy(pos_hbm.at[:, part], pos.at[:, part], in_sem.at[3 * c + 1]),
            pltpu.make_async_copy(vel_hbm.at[:, part], vel.at[:, part], in_sem.at[3 * c + 2]),
        ]
        for copy in group:
            copy.start()
        loads.append(group)

    lane = lax.broadcasted_iota(jnp.int32, (blocks, LANES), 1)
    row = lax.broadcasted_iota(jnp.int32, (blocks, 1), 0)
    packed = jnp.concatenate(
        [
            halo_ref[...].astype(F32),
            live_ref[...].astype(F32),
            shift_ref[...].astype(F32) * BOX,
            jnp.zeros((LANES - 5, blocks), F32),
        ],
        axis=0,
    )
    turned = packed.T
    live_col = jnp.where(row < count_ref[...], turned[:, 1:2], 0.0)
    cols[...] = jnp.where(lane == 1, live_col, turned)

    halo = turned[:, 0:1].astype(jnp.int32)
    home = home_ref[...]
    home_rows = home.shape[0]
    row_pick = lax.broadcasted_iota(jnp.int32, (blocks, home_rows), 1) == quotient(halo, LANES)
    split = jnp.concatenate([(home >> 8).astype(F32), (home & 255).astype(F32)], axis=1)
    picked = jnp.dot(
        row_pick.astype(F32).astype(BF16), split.astype(BF16), preferred_element_type=F32
    )
    value = picked[:, :LANES] * 256.0 + picked[:, LANES:]
    slot = jnp.sum(jnp.where(lane == (halo & (LANES - 1)), value, 0.0), axis=1, keepdims=True)
    slot = slot.astype(jnp.int32)
    owner = quotient(slot, owned)
    owner_grp = quotient(owner, domains)
    turn = owner - owner_grp * domains - d
    turn = jnp.where(turn < 0, turn + domains, turn)
    column = (jnp.where(owner_grp == g, 0, domains) + turn) * owned + slot - owner * owned
    spread_lanes = lax.broadcasted_iota(jnp.int32, (blocks, 2 * domains * owned), 1)
    onehot = (spread_lanes == column).astype(F32).astype(BF16)

    lane8 = lax.broadcasted_iota(jnp.int32, (8, LANES), 1)
    position8 = lax.broadcasted_iota(jnp.int32, (8, width), 1).astype(F32)

    def fold(x):
        parts = [x[:, i * LANES:(i + 1) * LANES] for i in range(width // LANES)]
        return jnp.sum(functools.reduce(lambda a, b: a + b, parts), axis=1, keepdims=True)

    def moment_rows(start):
        at = pl.ds(start, 8)
        col = cols[at]
        w = jnp.where(position8 < col[:, 1:2], mass[at], 0.0)
        u = [pos[k, at] + col[:, 2 + k:3 + k] for k in range(3)]
        v = [vel[k, at] for k in range(3)]
        wv = [w * x for x in v]
        made = [w] + [w * x for x in u] + wv
        made += [wv[0] * v[0] + wv[1] * v[1] + wv[2] * v[2]]
        made += list(crossed(u, wv))
        out = jnp.zeros((8, LANES), F32)
        for k, x in enumerate(made):
            out = jnp.where(lane8 == k, fold(x), out)
        moments[at] = out

    for c in range(CHUNKS):
        for copy in loads[c]:
            copy.wait()

        def step(i, carry, c=c):
            moment_rows(pl.multiple_of(c * rows + i * 8, 8))
            return carry

        lax.fori_loop(0, rows // 8, step, 0, unroll=True)

    by_row = moments[...].T[:16]
    mass_sum = jnp.sum(by_row[0:1], axis=1, keepdims=True)
    stacked = jnp.concatenate(pieces(by_row), axis=0).astype(BF16)
    product = jnp.dot(stacked, onehot, preferred_element_type=F32)
    product = product[:16] + product[16:32] + product[32:48]
    row8 = lax.broadcasted_iota(jnp.int32, (8, owned), 0)
    for dd in range(domains):
        for ahead in range(2):
            k = ahead * domains + dd
            tile = product[:, k * owned:(k + 1) * owned]
            tables[dd, ahead] = tile[:8]
            tables[dd, 2 + ahead] = jnp.where(row8 == MASS_ROW - 8, mass_sum, tile[8:])

    pl.semaphore_wait(barrier, len(partners))

    first = {}
    for dd in range(1, domains):
        first[dd] = remote(
            tables.at[dd], parts_in.at[dd], send1.at[dd], recv1.at[dd], 0, dd
        )
        first[dd].start()
    total_of = [tables[0, q] for q in range(4)]
    for dd in range(1, domains):
        first[dd].wait_recv()
        total_of = [total_of[q] + parts_in[dd, q] for q in range(4)]
    own[...] = jnp.stack(total_of, axis=0)
    mine, ahead = own.at[0], own.at[1]

    second = []
    for dd in list(range(1, domains)) + [0]:
        second.append(
            remote(ahead, behind_in.at[dd], send_up.at[dd], recv_up.at[dd], 1, -dd)
        )
        second.append(
            remote(mine, ahead_in.at[dd], send_down.at[dd], recv_down.at[dd], -1, -dd)
        )
    for dd in range(1, domains):
        second.append(
            remote(own.at[pl.ds(0, 2)], near_in.at[dd], send_near.at[dd], recv_near.at[dd], 0, -dd)
        )
    late = [remote(own.at[3], rest_in, send_rest, recv_rest, 1, 0)]
    for dg in range(1, groups):
        late.append(
            remote(
                own.at[2, pl.ds(MASS_ROW - 8, 1)], totals_in.at[dg],
                send_total.at[dg], recv_total.at[dg], dg, 0,
            )
        )
    for copy in second + late:
        copy.start()
    for copy in second:
        copy.wait_recv()

    here, there = [], []
    for dd in range(domains):
        near = [total_of[0], total_of[1]] if dd == 0 else [near_in[dd, 0], near_in[dd, 1]]
        here.append(near[0] + behind_in[dd])
        there.append(near[1] + ahead_in[dd])
    every = jnp.concatenate(here + there, axis=1)
    stacked = jnp.concatenate(list(pieces(every)) + [jnp.zeros_like(every)], axis=0).astype(BF16)
    gathered = lax.dot_general(
        stacked, onehot, (((1,), (1,)), ((), ())), preferred_element_type=F32
    )
    gathered = gathered[0:8] + gathered[8:16] + gathered[16:24]
    centre, drift, spread = halo_means(gathered)
    shifts = packed[2:5]
    live = jnp.where(
        lax.broadcasted_iota(jnp.int32, (1, blocks), 1) < count_ref[...], packed[1:2], 0.0
    )
    by_block = jnp.concatenate(
        [centre[k] - shifts[k:k + 1] for k in range(3)]
        + drift
        + [1.0 / (3.0 * spread + EPSILON), live, jnp.zeros((LANES - 8, blocks), F32)],
        axis=0,
    )
    means_ref[...] = by_block.T

    for copy in late:
        copy.wait_recv()
    total = total_of[2][MASS_ROW - 8:MASS_ROW - 7]
    for dg in range(1, groups):
        total = total + totals_in[dg]
    sums_ref[0:8] = here[0]
    sums_ref[8:16] = jnp.where(row8 == MASS_ROW - 8, total, total_of[2] + rest_in[...])

    for copy in list(first.values()) + second + late:
        copy.wait_send()


def halo_means(sums):
    scaled = sums[1:8] * (1.0 / jnp.maximum(sums[0:1], 1.0))
    centre = [scaled[k:k + 1] for k in range(3)]
    drift = [scaled[3 + k:4 + k] for k in range(3)]
    spread = scaled[6:7] - (drift[0] * drift[0] + drift[1] * drift[1] + drift[2] * drift[2])
    return centre, drift, spread


def output_kernel(
    halos, pos, vel, means_ref, sums_ref, table_hbm, kin_hbm, rad_hbm, table, kin, rad, sem
):
    blocks, width = kin.shape
    rows = blocks // CHUNKS
    position8 = lax.broadcasted_iota(jnp.int32, (8, width), 1).astype(F32)

    sums = sums_ref[...]
    centre, drift, spread = halo_means(sums)
    heavy_inv = 1.0 / jnp.maximum(sums[0:1], 1.0)
    turned_spin = crossed(centre, drift)
    spin = [sums[8 + k:9 + k] * heavy_inv - turned_spin[k] for k in range(3)]
    share = sums[0:1] * float(halos) / sums[MASS_ROW:MASS_ROW + 1]
    table[...] = jnp.concatenate([share] + centre + drift + [spread] + spin, axis=0)
    stores = [pltpu.make_async_copy(table, table_hbm, sem.at[2 * CHUNKS])]
    stores[0].start()

    def output_rows(start):
        at = pl.ds(start, 8)
        mean = means_ref[at]
        live = position8 < mean[:, 7:8]
        kinetic = 0.0
        radial = 0.0
        for k in range(3):
            distance = pos[k, at] - mean[:, k:k + 1]
            radial = radial + distance * distance
            offset = vel[k, at] - mean[:, 3 + k:4 + k]
            kinetic = kinetic + offset * offset
        kin[at] = jnp.where(live, kinetic * mean[:, 6:7], 0.0)
        rad[at] = jnp.where(live, radial, 0.0)

    for c in range(CHUNKS):

        def step(i, carry, c=c):
            output_rows(pl.multiple_of(c * rows + i * 8, 8))
            return carry

        lax.fori_loop(0, rows // 8, step, 0, unroll=True)
        part = pl.ds(c * rows, rows)
        group = [
            pltpu.make_async_copy(kin.at[part], kin_hbm.at[part], sem.at[2 * c]),
            pltpu.make_async_copy(rad.at[part], rad_hbm.at[part], sem.at[2 * c + 1]),
        ]
        for copy in group:
            copy.start()
        stores += group
    for copy in stores:
        copy.wait()


def solution(mesh):
    groups, domains = mesh.shape["grp"], mesh.shape["dom"]

    def local(
        positions, velocities, masses, block_halo, block_shift, block_live, block_count, home_slot
    ):
        blocks, width = masses.shape
        halos = home_slot.shape[0]
        owned = halos // (groups * domains)
        vmem = pl.BlockSpec(memory_space=pltpu.VMEM)
        hbm = pl.BlockSpec(memory_space=pl.ANY)
        dma = pltpu.SemaphoreType.DMA
        pos, vel, means, sums = pl.pallas_call(
            functools.partial(exchange_kernel, groups, domains, owned),
            out_shape=(
                pltpu.VMEM((3, blocks, width), F32),
                pltpu.VMEM((3, blocks, width), F32),
                pltpu.VMEM((blocks, LANES), F32),
                pltpu.VMEM((16, owned), F32),
            ),
            in_specs=[hbm, hbm, hbm, vmem, vmem, vmem, vmem, vmem],
            out_specs=(vmem, vmem, vmem, vmem),
            scratch_shapes=[
                pltpu.VMEM((blocks, width), F32),
                pltpu.VMEM((blocks, LANES), F32),
                pltpu.VMEM((blocks, LANES), F32),
                pltpu.VMEM((domains, 4, 8, owned), F32),
                pltpu.VMEM((domains, 4, 8, owned), F32),
                pltpu.VMEM((4, 8, owned), F32),
                pltpu.VMEM((domains, 2, 8, owned), F32),
                pltpu.VMEM((domains, 8, owned), F32),
                pltpu.VMEM((domains, 8, owned), F32),
                pltpu.VMEM((8, owned), F32),
                pltpu.VMEM((groups, 1, owned), F32),
                dma((3 * CHUNKS,)),
                dma((domains,)), dma((domains,)),
                dma((domains,)), dma((domains,)),
                dma((domains,)), dma((domains,)),
                dma((domains,)), dma((domains,)),
                dma, dma,
                dma((groups,)), dma((groups,)),
            ],
            compiler_params=pltpu.CompilerParams(collective_id=0, has_side_effects=True),
        )(
            positions, velocities, masses,
            block_halo.reshape(1, blocks), block_shift, block_live.reshape(1, blocks),
            block_count.reshape(1, 1), home_slot.reshape(halos // LANES, LANES),
        )
        return pl.pallas_call(
            functools.partial(output_kernel, halos),
            out_shape=(
                jax.ShapeDtypeStruct((11, owned), F32),
                jax.ShapeDtypeStruct((blocks, width), F32),
                jax.ShapeDtypeStruct((blocks, width), F32),
            ),
            in_specs=[vmem, vmem, vmem, vmem],
            out_specs=(hbm, hbm, hbm),
            scratch_shapes=[
                pltpu.VMEM((11, owned), F32),
                pltpu.VMEM((blocks, width), F32),
                pltpu.VMEM((blocks, width), F32),
                dma((2 * CHUNKS + 1,)),
            ],
        )(*[pltpu.with_memory_space_constraint(x, pltpu.VMEM) for x in (pos, vel, means, sums)])

    return jax.shard_map(
        local,
        mesh=mesh,
        in_specs=(
            P(None, ("grp", "dom"), None),
            P(None, ("grp", "dom"), None),
            P(("grp", "dom"), None),
            P(("grp", "dom")),
            P(None, ("grp", "dom")),
            P(("grp", "dom")),
            P(("grp", "dom")),
            P(),
        ),
        out_specs=(P(None, ("grp", "dom")), P(("grp", "dom"), None), P(("grp", "dom"), None)),
        check_vma=False,
    )
```

```python
import functools

import jax
import jax.numpy as jnp
from jax import lax
from jax.experimental import pallas as pl
from jax.experimental.pallas import tpu as pltpu
from jax.sharding import PartitionSpec as P

BOX = 1.0
EPSILON = 1e-06
MESH = pl.DeviceIdType.MESH
F32 = jnp.float32
BF16 = jnp.bfloat16
LANES = 128
CHUNKS = 4
MASS_ROW = 11


def pieces(x):
    hi = x.astype(BF16).astype(F32)
    rest = x - hi
    mid = rest.astype(BF16).astype(F32)
    return hi, mid, rest - mid


def quotient(x, n):
    return x >> (n.bit_length() - 1) if n & (n - 1) == 0 else x // n


def crossed(a, b):
    return (a[1] * b[2] - a[2] * b[1], a[2] * b[0] - a[0] * b[2], a[0] * b[1] - a[1] * b[0])


def exchange_kernel(
    groups, domains, owned,
    pos_hbm, vel_hbm, mass_hbm, halo_hbm, shift_hbm, live_hbm, count_ref, home_hbm,
    pos, vel, means_ref, sums_ref,
    halo_ref, shift_ref, live_ref, home_ref, small_sem, mass, cols, moments, tables, parts_in, own, own_rest, near_in, ahead_in, behind_in, rest_in, totals_in,
    in_sem, send1, recv1, send1b, recv1b, send_near, recv_near, send_up, recv_up, send_down, recv_down,
    send_rest, recv_rest, send_total, recv_total,
):
    blocks, width = mass.shape
    rows = blocks // CHUNKS
    g = lax.axis_index("grp")
    d = lax.axis_index("dom")

    def peer(dg, dd):
        return {"grp": lax.rem(g + dg % groups, groups), "dom": lax.rem(d + dd % domains, domains)}

    def remote(src, dst, send, recv, dg, dd):
        return pltpu.make_async_remote_copy(
            src_ref=src, dst_ref=dst, send_sem=send, recv_sem=recv,
            device_id=peer(dg, dd), device_id_type=MESH,
        )

    pairs = ((halo_hbm, halo_ref), (live_hbm, live_ref), (shift_hbm, shift_ref), (home_hbm, home_ref))
    smalls = [
        pltpu.make_async_copy(src, dst, small_sem.at[k]) for k, (src, dst) in enumerate(pairs)
    ]
    for copy in smalls:
        copy.start()
    loads = []
    for c in range(CHUNKS):
        part = pl.ds(c * rows, rows)
        group = [
            pltpu.make_async_copy(mass_hbm.at[part], mass.at[part], in_sem.at[3 * c]),
            pltpu.make_async_copy(pos_hbm.at[:, part], pos.at[:, part], in_sem.at[3 * c + 1]),
            pltpu.make_async_copy(vel_hbm.at[:, part], vel.at[:, part], in_sem.at[3 * c + 2]),
        ]
        for copy in group:
            copy.start()
        loads.append(group)

    partners = {(0, dd) for dd in range(domains)}
    partners |= {(1 % groups, dd) for dd in range(domains)}
    partners |= {(-1 % groups, dd) for dd in range(domains)}
    partners |= {(dg, 0) for dg in range(groups)}
    partners = sorted(partners - {(0, 0)})
    barrier = pltpu.get_barrier_semaphore()
    for dg, dd in partners:
        pl.semaphore_signal(barrier, inc=1, device_id=peer(dg, dd), device_id_type=MESH)

    for copy in smalls:
        copy.wait()

    lane = lax.broadcasted_iota(jnp.int32, (blocks, LANES), 1)
    row = lax.broadcasted_iota(jnp.int32, (blocks, 1), 0)
    packed = jnp.concatenate(
        [
            halo_ref[...].astype(F32),
            live_ref[...].astype(F32),
            shift_ref[...].astype(F32) * BOX,
            jnp.zeros((LANES - 5, blocks), F32),
        ],
        axis=0,
    )
    turned = packed.T
    live_col = jnp.where(row < count_ref[...], turned[:, 1:2], 0.0)
    cols[...] = jnp.where(lane == 1, live_col, turned)

    halo = turned[:, 0:1].astype(jnp.int32)
    home = home_ref[...]
    home_rows = home.shape[0]
    row_pick = lax.broadcasted_iota(jnp.int32, (blocks, home_rows), 1) == quotient(halo, LANES)
    split = jnp.concatenate([(home >> 8).astype(F32), (home & 255).astype(F32)], axis=1)
    picked = jnp.dot(
        row_pick.astype(F32).astype(BF16), split.astype(BF16), preferred_element_type=F32
    )
    value = picked[:, :LANES] * 256.0 + picked[:, LANES:]
    slot = jnp.sum(jnp.where(lane == (halo & (LANES - 1)), value, 0.0), axis=1, keepdims=True)
    slot = slot.astype(jnp.int32)
    owner = quotient(slot, owned)
    owner_grp = quotient(owner, domains)
    turn = owner - owner_grp * domains - d
    turn = jnp.where(turn < 0, turn + domains, turn)
    column = (jnp.where(owner_grp == g, 0, domains) + turn) * owned + slot - owner * owned
    spread_lanes = lax.broadcasted_iota(jnp.int32, (blocks, 2 * domains * owned), 1)
    onehot = (spread_lanes == column).astype(F32).astype(BF16)

    lane8 = lax.broadcasted_iota(jnp.int32, (8, LANES), 1)
    position8 = lax.broadcasted_iota(jnp.int32, (8, width), 1).astype(F32)

    def fold(x):
        parts = [x[:, i * LANES:(i + 1) * LANES] for i in range(width // LANES)]
        return jnp.sum(functools.reduce(lambda a, b: a + b, parts), axis=1, keepdims=True)

    def moment_rows(start):
        at = pl.ds(start, 8)
        col = cols[at]
        w = jnp.where(position8 < col[:, 1:2], mass[at], 0.0)
        u = [pos[k, at] + col[:, 2 + k:3 + k] for k in range(3)]
        v = [vel[k, at] for k in range(3)]
        wv = [w * x for x in v]
        made = [w] + [w * x for x in u] + wv
        made += [wv[0] * v[0] + wv[1] * v[1] + wv[2] * v[2]]
        made += list(crossed(u, wv))
        out = jnp.zeros((8, LANES), F32)
        for k, x in enumerate(made):
            out = jnp.where(lane8 == k, fold(x), out)
        moments[at] = out

    for c in range(CHUNKS):
        for copy in loads[c]:
            copy.wait()

        def step(i, carry, c=c):
            moment_rows(pl.multiple_of(c * rows + i * 8, 8))
            return carry

        lax.fori_loop(0, rows // 8, step, 0, unroll=True)

    by_row = moments[...].T[:16]
    mass_sum = jnp.sum(by_row[0:1], axis=1, keepdims=True)
    stacked = jnp.concatenate(pieces(by_row), axis=0).astype(BF16)
    product = jnp.dot(stacked, onehot, preferred_element_type=F32)
    product = product[:16] + product[16:32] + product[32:48]
    row8 = lax.broadcasted_iota(jnp.int32, (8, owned), 0)
    for dd in range(domains):
        for ahead in range(2):
            k = ahead * domains + dd
            tile = product[:, k * owned:(k + 1) * owned]
            tables[dd, ahead] = tile[:8]
            tables[dd, 2 + ahead] = jnp.where(row8 == MASS_ROW - 8, mass_sum, tile[8:])

    pl.semaphore_wait(barrier, len(partners))

    first, other = {}, {}
    for part, copies, send, recv in ((0, first, send1, recv1), (2, other, send1b, recv1b)):
        for dd in range(1, domains):
            copies[dd] = remote(
                tables.at[dd, pl.ds(part, 2)], parts_in.at[dd, pl.ds(part, 2)],
                send.at[dd], recv.at[dd], 0, dd,
            )
            copies[dd].start()
    total_of = [tables[0, q] for q in range(4)]
    for dd in range(1, domains):
        first[dd].wait_recv()
        for q in range(2):
            total_of[q] = total_of[q] + parts_in[dd, q]
    own[...] = jnp.stack(total_of[:2], axis=0)
    mine, ahead = own.at[0], own.at[1]

    second = []
    for dd in list(range(1, domains)) + [0]:
        second.append(
            remote(ahead, behind_in.at[dd], send_up.at[dd], recv_up.at[dd], 1, -dd)
        )
        second.append(
            remote(mine, ahead_in.at[dd], send_down.at[dd], recv_down.at[dd], -1, -dd)
        )
    for dd in range(1, domains):
        second.append(
            remote(own, near_in.at[dd], send_near.at[dd], recv_near.at[dd], 0, -dd)
        )
    for copy in second:
        copy.start()
    for dd in range(1, domains):
        other[dd].wait_recv()
        for q in range(2, 4):
            total_of[q] = total_of[q] + parts_in[dd, q]
    own_rest[...] = jnp.stack(total_of[2:], axis=0)
    late = []
    for dg in range(1, groups):
        late.append(
            remote(
                own_rest.at[0, pl.ds(MASS_ROW - 8, 1)], totals_in.at[dg],
                send_total.at[dg], recv_total.at[dg], dg, 0,
            )
        )
    late.append(remote(own_rest.at[1], rest_in, send_rest, recv_rest, 1, 0))
    for copy in late:
        copy.start()
    for copy in second:
        copy.wait_recv()

    here, there = [], []
    for dd in range(domains):
        near = [total_of[0], total_of[1]] if dd == 0 else [near_in[dd, 0], near_in[dd, 1]]
        here.append(near[0] + behind_in[dd])
        there.append(near[1] + ahead_in[dd])
    every = jnp.concatenate(here + there, axis=1)
    stacked = jnp.concatenate(list(pieces(every)) + [jnp.zeros_like(every)], axis=0).astype(BF16)
    gathered = lax.dot_general(
        stacked, onehot, (((1,), (1,)), ((), ())), preferred_element_type=F32
    )
    gathered = gathered[0:8] + gathered[8:16] + gathered[16:24]
    centre, drift, spread = halo_means(gathered)
    shifts = packed[2:5]
    live = jnp.where(
        lax.broadcasted_iota(jnp.int32, (1, blocks), 1) < count_ref[...], packed[1:2], 0.0
    )
    by_block = jnp.concatenate(
        [centre[k] - shifts[k:k + 1] for k in range(3)]
        + drift
        + [1.0 / (3.0 * spread + EPSILON), live, jnp.zeros((LANES - 8, blocks), F32)],
        axis=0,
    )
    means_ref[...] = by_block.T

    for copy in late:
        copy.wait_recv()
    total = total_of[2][MASS_ROW - 8:MASS_ROW - 7]
    for dg in range(1, groups):
        total = total + totals_in[dg]
    sums_ref[0:8] = here[0]
    sums_ref[8:16] = jnp.where(row8 == MASS_ROW - 8, total, total_of[2] + rest_in[...])

    for copy in list(first.values()) + list(other.values()) + second + late:
        copy.wait_send()


def halo_means(sums):
    scaled = sums[1:8] * (1.0 / jnp.maximum(sums[0:1], 1.0))
    centre = [scaled[k:k + 1] for k in range(3)]
    drift = [scaled[3 + k:4 + k] for k in range(3)]
    spread = scaled[6:7] - (drift[0] * drift[0] + drift[1] * drift[1] + drift[2] * drift[2])
    return centre, drift, spread


def output_kernel(
    halos, pos, vel, means_ref, sums_ref, table_hbm, kin_hbm, rad_hbm, table, kin, rad, sem
):
    blocks, width = kin.shape
    rows = blocks // CHUNKS
    position8 = lax.broadcasted_iota(jnp.int32, (8, width), 1).astype(F32)

    sums = sums_ref[...]
    centre, drift, spread = halo_means(sums)
    heavy_inv = 1.0 / jnp.maximum(sums[0:1], 1.0)
    turned_spin = crossed(centre, drift)
    spin = [sums[8 + k:9 + k] * heavy_inv - turned_spin[k] for k in range(3)]
    share = sums[0:1] * float(halos) / sums[MASS_ROW:MASS_ROW + 1]
    table[...] = jnp.concatenate([share] + centre + drift + [spread] + spin, axis=0)
    stores = [pltpu.make_async_copy(table, table_hbm, sem.at[2 * CHUNKS])]
    stores[0].start()

    def output_rows(start):
        at = pl.ds(start, 8)
        mean = means_ref[at]
        live = position8 < mean[:, 7:8]
        kinetic = 0.0
        radial = 0.0
        for k in range(3):
            distance = pos[k, at] - mean[:, k:k + 1]
            radial = radial + distance * distance
            offset = vel[k, at] - mean[:, 3 + k:4 + k]
            kinetic = kinetic + offset * offset
        kin[at] = jnp.where(live, kinetic * mean[:, 6:7], 0.0)
        rad[at] = jnp.where(live, radial, 0.0)

    for c in range(CHUNKS):

        def step(i, carry, c=c):
            output_rows(pl.multiple_of(c * rows + i * 8, 8))
            return carry

        lax.fori_loop(0, rows // 8, step, 0, unroll=True)
        part = pl.ds(c * rows, rows)
        group = [
            pltpu.make_async_copy(kin.at[part], kin_hbm.at[part], sem.at[2 * c]),
            pltpu.make_async_copy(rad.at[part], rad_hbm.at[part], sem.at[2 * c + 1]),
        ]
        for copy in group:
            copy.start()
        stores += group
    for copy in stores:
        copy.wait()


def solution(mesh):
    groups, domains = mesh.shape["grp"], mesh.shape["dom"]

    def local(
        positions, velocities, masses, block_halo, block_shift, block_live, block_count, home_slot
    ):
        blocks, width = masses.shape
        halos = home_slot.shape[0]
        owned = halos // (groups * domains)
        vmem = pl.BlockSpec(memory_space=pltpu.VMEM)
        hbm = pl.BlockSpec(memory_space=pl.ANY)
        dma = pltpu.SemaphoreType.DMA
        pos, vel, means, sums = pl.pallas_call(
            functools.partial(exchange_kernel, groups, domains, owned),
            out_shape=(
                pltpu.VMEM((3, blocks, width), F32),
                pltpu.VMEM((3, blocks, width), F32),
                pltpu.VMEM((blocks, LANES), F32),
                pltpu.VMEM((16, owned), F32),
            ),
            in_specs=[hbm, hbm, hbm, hbm, hbm, hbm, vmem, hbm],
            out_specs=(vmem, vmem, vmem, vmem),
            scratch_shapes=[
                pltpu.VMEM((1, blocks), jnp.int32),
                pltpu.VMEM((3, blocks), jnp.int32),
                pltpu.VMEM((1, blocks), jnp.int32),
                pltpu.VMEM((halos // LANES, LANES), jnp.int32),
                dma((4,)),
                pltpu.VMEM((blocks, width), F32),
                pltpu.VMEM((blocks, LANES), F32),
                pltpu.VMEM((blocks, LANES), F32),
                pltpu.VMEM((domains, 4, 8, owned), F32),
                pltpu.VMEM((domains, 4, 8, owned), F32),
                pltpu.VMEM((2, 8, owned), F32),
                pltpu.VMEM((2, 8, owned), F32),
                pltpu.VMEM((domains, 2, 8, owned), F32),
                pltpu.VMEM((domains, 8, owned), F32),
                pltpu.VMEM((domains, 8, owned), F32),
                pltpu.VMEM((8, owned), F32),
                pltpu.VMEM((groups, 1, owned), F32),
                dma((3 * CHUNKS,)),
                dma((domains,)), dma((domains,)),
                dma((domains,)), dma((domains,)),
                dma((domains,)), dma((domains,)),
                dma((domains,)), dma((domains,)),
                dma((domains,)), dma((domains,)),
                dma, dma,
                dma((groups,)), dma((groups,)),
            ],
            compiler_params=pltpu.CompilerParams(collective_id=0, has_side_effects=True),
        )(
            positions, velocities, masses,
            block_halo.reshape(1, blocks), block_shift, block_live.reshape(1, blocks),
            block_count.reshape(1, 1), home_slot.reshape(halos // LANES, LANES),
        )
        return pl.pallas_call(
            functools.partial(output_kernel, halos),
            out_shape=(
                jax.ShapeDtypeStruct((11, owned), F32),
                jax.ShapeDtypeStruct((blocks, width), F32),
                jax.ShapeDtypeStruct((blocks, width), F32),
            ),
            in_specs=[vmem, vmem, vmem, vmem],
            out_specs=(hbm, hbm, hbm),
            scratch_shapes=[
                pltpu.VMEM((11, owned), F32),
                pltpu.VMEM((blocks, width), F32),
                pltpu.VMEM((blocks, width), F32),
                dma((2 * CHUNKS + 1,)),
            ],
        )(*[pltpu.with_memory_space_constraint(x, pltpu.VMEM) for x in (pos, vel, means, sums)])

    return jax.shard_map(
        local,
        mesh=mesh,
        in_specs=(
            P(None, ("grp", "dom"), None),
            P(None, ("grp", "dom"), None),
            P(("grp", "dom"), None),
            P(("grp", "dom")),
            P(None, ("grp", "dom")),
            P(("grp", "dom")),
            P(("grp", "dom")),
            P(),
        ),
        out_specs=(P(None, ("grp", "dom")), P(("grp", "dom"), None), P(("grp", "dom"), None)),
        check_vma=False,
    )
```

```python
import functools

import jax
import jax.numpy as jnp
from jax import lax
from jax.experimental import pallas as pl
from jax.experimental.pallas import tpu as pltpu
from jax.sharding import PartitionSpec as P

BOX = 1.0
EPSILON = 1e-06
MESH = pl.DeviceIdType.MESH
F32 = jnp.float32
BF16 = jnp.bfloat16
LANES = 128
CHUNKS = 2
MASS_ROW = 11


def pieces(x):
    hi = x.astype(BF16).astype(F32)
    rest = x - hi
    mid = rest.astype(BF16).astype(F32)
    return hi, mid, rest - mid


def quotient(x, n):
    return x >> (n.bit_length() - 1) if n & (n - 1) == 0 else x // n


def crossed(a, b):
    return (a[1] * b[2] - a[2] * b[1], a[2] * b[0] - a[0] * b[2], a[0] * b[1] - a[1] * b[0])


def exchange_kernel(
    groups, domains, owned,
    pos_hbm, vel_hbm, mass_hbm, halo_hbm, shift_hbm, live_hbm, count_ref, home_hbm,
    pos, vel, means_ref, sums_ref,
    halo_ref, shift_ref, live_ref, home_ref, small_sem, mass, cols, moments, tables, parts_in, own, own_rest, total_out, near_in, ahead_in, behind_in, rest_in, totals_in,
    in_sem, send1, recv1, send1b, recv1b, send_near, recv_near, send_up, recv_up, send_down, recv_down,
    send_rest, recv_rest, send_total, recv_total,
):
    blocks, width = mass.shape
    rows = blocks // CHUNKS
    g = lax.axis_index("grp")
    d = lax.axis_index("dom")

    def peer(dg, dd):
        return {"grp": lax.rem(g + dg % groups, groups), "dom": lax.rem(d + dd % domains, domains)}

    def remote(src, dst, send, recv, dg, dd):
        return pltpu.make_async_remote_copy(
            src_ref=src, dst_ref=dst, send_sem=send, recv_sem=recv,
            device_id=peer(dg, dd), device_id_type=MESH,
        )

    pairs = ((halo_hbm, halo_ref), (live_hbm, live_ref), (shift_hbm, shift_ref), (home_hbm, home_ref))
    smalls = [
        pltpu.make_async_copy(src, dst, small_sem.at[k]) for k, (src, dst) in enumerate(pairs)
    ]
    for copy in smalls:
        copy.start()
    loads = []
    for c in range(CHUNKS):
        part = pl.ds(c * rows, rows)
        group = [
            pltpu.make_async_copy(mass_hbm.at[part], mass.at[part], in_sem.at[3 * c]),
            pltpu.make_async_copy(pos_hbm.at[:, part], pos.at[:, part], in_sem.at[3 * c + 1]),
            pltpu.make_async_copy(vel_hbm.at[:, part], vel.at[:, part], in_sem.at[3 * c + 2]),
        ]
        for n, copy in enumerate(group):
            copy.start(priority=(c + n) % 2)
        loads.append(group)

    partners = {(0, dd) for dd in range(domains)}
    partners |= {(1 % groups, dd) for dd in range(domains)}
    partners |= {(-1 % groups, dd) for dd in range(domains)}
    partners |= {(dg, 0) for dg in range(groups)}
    partners = sorted(partners - {(0, 0)})
    barrier = pltpu.get_barrier_semaphore()
    for dg, dd in partners:
        pl.semaphore_signal(barrier, inc=1, device_id=peer(dg, dd), device_id_type=MESH)

    for copy in smalls:
        copy.wait()

    lane = lax.broadcasted_iota(jnp.int32, (blocks, LANES), 1)
    row = lax.broadcasted_iota(jnp.int32, (blocks, 1), 0)
    packed = jnp.concatenate(
        [
            halo_ref[...].astype(F32),
            live_ref[...].astype(F32),
            shift_ref[...].astype(F32) * BOX,
            jnp.zeros((LANES - 5, blocks), F32),
        ],
        axis=0,
    )
    turned = packed.T
    live_col = jnp.where(row < count_ref[...], turned[:, 1:2], 0.0)
    cols[...] = jnp.where(lane == 1, live_col, turned)

    halo = turned[:, 0:1].astype(jnp.int32)
    home = home_ref[...]
    home_rows = home.shape[0]
    row_pick = lax.broadcasted_iota(jnp.int32, (blocks, home_rows), 1) == quotient(halo, LANES)
    split = jnp.concatenate([(home >> 8).astype(F32), (home & 255).astype(F32)], axis=1)
    picked = jnp.dot(
        row_pick.astype(F32).astype(BF16), split.astype(BF16), preferred_element_type=F32
    )
    value = picked[:, :LANES] * 256.0 + picked[:, LANES:]
    slot = jnp.sum(jnp.where(lane == (halo & (LANES - 1)), value, 0.0), axis=1, keepdims=True)
    slot = slot.astype(jnp.int32)
    owner = quotient(slot, owned)
    owner_grp = quotient(owner, domains)
    turn = owner - owner_grp * domains - d
    turn = jnp.where(turn < 0, turn + domains, turn)
    column = (jnp.where(owner_grp == g, 0, domains) + turn) * owned + slot - owner * owned
    spread_lanes = lax.broadcasted_iota(jnp.int32, (blocks, 2 * domains * owned), 1)
    onehot = (spread_lanes == column).astype(F32).astype(BF16)

    lane8 = lax.broadcasted_iota(jnp.int32, (8, LANES), 1)
    position8 = lax.broadcasted_iota(jnp.int32, (8, width), 1).astype(F32)

    def fold(x):
        parts = [x[:, i * LANES:(i + 1) * LANES] for i in range(width // LANES)]
        return jnp.sum(functools.reduce(lambda a, b: a + b, parts), axis=1, keepdims=True)

    def moment_rows(start):
        at = pl.ds(start, 8)
        col = cols[at]
        w = jnp.where(position8 < col[:, 1:2], mass[at], 0.0)
        u = [pos[k, at] + col[:, 2 + k:3 + k] for k in range(3)]
        v = [vel[k, at] for k in range(3)]
        wv = [w * x for x in v]
        made = [w] + [w * x for x in u] + wv
        made += [wv[0] * v[0] + wv[1] * v[1] + wv[2] * v[2]]
        made += list(crossed(u, wv))
        out = jnp.zeros((8, LANES), F32)
        for k, x in enumerate(made):
            out = jnp.where(lane8 == k, fold(x), out)
        moments[at] = out

    for c in range(CHUNKS):
        for copy in loads[c]:
            copy.wait()

        def step(i, carry, c=c):
            moment_rows(pl.multiple_of(c * rows + i * 8, 8))
            return carry

        lax.fori_loop(0, rows // 8, step, 0, unroll=True)

    by_row = moments[...].T[:16]
    mass_sum = jnp.sum(by_row[0:1], axis=1, keepdims=True)
    stacked = jnp.concatenate(pieces(by_row), axis=0).astype(BF16)
    product = jnp.dot(stacked, onehot, preferred_element_type=F32)
    product = product[:16] + product[16:32] + product[32:48]
    row8 = lax.broadcasted_iota(jnp.int32, (8, owned), 0)
    for dd in range(domains):
        for ahead in range(2):
            k = ahead * domains + dd
            tile = product[:, k * owned:(k + 1) * owned]
            tables[dd, ahead] = tile[:8]
            tables[dd, 2 + ahead] = jnp.where(row8 == MASS_ROW - 8, mass_sum, tile[8:])

    pl.semaphore_wait(barrier, len(partners))

    first, other = {}, {}
    for part, size, copies, send, recv in ((0, 3, first, send1, recv1), (3, 1, other, send1b, recv1b)):
        for dd in range(1, domains):
            copies[dd] = remote(
                tables.at[dd, pl.ds(part, size)], parts_in.at[dd, pl.ds(part, size)],
                send.at[dd], recv.at[dd], 0, dd,
            )
            copies[dd].start()
    total_of = [tables[0, q] for q in range(4)]
    for dd in range(1, domains):
        first[dd].wait_recv()
        for q in range(3):
            total_of[q] = total_of[q] + parts_in[dd, q]
    own[...] = jnp.stack(total_of[:2], axis=0)
    total_out[0] = total_of[2][MASS_ROW - 8:MASS_ROW - 7]
    mine, ahead = own.at[0], own.at[1]

    second = []
    for dd in list(range(1, domains)) + [0]:
        second.append(
            remote(ahead, behind_in.at[dd], send_up.at[dd], recv_up.at[dd], 1, -dd)
        )
        second.append(
            remote(mine, ahead_in.at[dd], send_down.at[dd], recv_down.at[dd], -1, -dd)
        )
    for dd in range(1, domains):
        second.append(
            remote(own, near_in.at[dd], send_near.at[dd], recv_near.at[dd], 0, -dd)
        )
    late = []
    for dg in sorted(range(1, groups), key=lambda x: -min(x, groups - x)):
        late.append(
            remote(
                total_out.at[0], totals_in.at[dg],
                send_total.at[dg], recv_total.at[dg], dg, 0,
            )
        )
    for copy in late + second:
        copy.start()
    for dd in range(1, domains):
        other[dd].wait_recv()
        total_of[3] = total_of[3] + parts_in[dd, 3]
    own_rest[...] = total_of[3]
    late.append(remote(own_rest, rest_in, send_rest, recv_rest, 1, 0))
    late[-1].start()
    for copy in second:
        copy.wait_recv()

    here, there = [], []
    for dd in range(domains):
        near = [total_of[0], total_of[1]] if dd == 0 else [near_in[dd, 0], near_in[dd, 1]]
        here.append(near[0] + behind_in[dd])
        there.append(near[1] + ahead_in[dd])
    every = jnp.concatenate(here + there, axis=1)
    stacked = jnp.concatenate(list(pieces(every)) + [jnp.zeros_like(every)], axis=0).astype(BF16)
    gathered = lax.dot_general(
        stacked, onehot, (((1,), (1,)), ((), ())), preferred_element_type=F32
    )
    gathered = gathered[0:8] + gathered[8:16] + gathered[16:24]
    centre, drift, spread = halo_means(gathered)
    shifts = packed[2:5]
    live = jnp.where(
        lax.broadcasted_iota(jnp.int32, (1, blocks), 1) < count_ref[...], packed[1:2], 0.0
    )
    by_block = jnp.concatenate(
        [centre[k] - shifts[k:k + 1] for k in range(3)]
        + drift
        + [1.0 / (3.0 * spread + EPSILON), live, jnp.zeros((LANES - 8, blocks), F32)],
        axis=0,
    )
    means_ref[...] = by_block.T

    for copy in late:
        copy.wait_recv()
    total = total_of[2][MASS_ROW - 8:MASS_ROW - 7]
    for dg in range(1, groups):
        total = total + totals_in[dg]
    sums_ref[0:8] = here[0]
    sums_ref[8:16] = jnp.where(row8 == MASS_ROW - 8, total, total_of[2] + rest_in[...])

    for copy in list(first.values()) + list(other.values()) + second + late:
        copy.wait_send()


def halo_means(sums):
    scaled = sums[1:8] * (1.0 / jnp.maximum(sums[0:1], 1.0))
    centre = [scaled[k:k + 1] for k in range(3)]
    drift = [scaled[3 + k:4 + k] for k in range(3)]
    spread = scaled[6:7] - (drift[0] * drift[0] + drift[1] * drift[1] + drift[2] * drift[2])
    return centre, drift, spread


def output_kernel(
    halos, pos, vel, means_ref, sums_ref, table_hbm, kin_hbm, rad_hbm, table, kin, rad, sem
):
    blocks, width = kin.shape
    rows = blocks // CHUNKS
    position8 = lax.broadcasted_iota(jnp.int32, (8, width), 1).astype(F32)

    sums = sums_ref[...]
    centre, drift, spread = halo_means(sums)
    heavy_inv = 1.0 / jnp.maximum(sums[0:1], 1.0)
    turned_spin = crossed(centre, drift)
    spin = [sums[8 + k:9 + k] * heavy_inv - turned_spin[k] for k in range(3)]
    share = sums[0:1] * float(halos) / sums[MASS_ROW:MASS_ROW + 1]
    table[...] = jnp.concatenate([share] + centre + drift + [spread] + spin, axis=0)
    stores = [pltpu.make_async_copy(table, table_hbm, sem.at[2 * CHUNKS])]
    stores[0].start()

    def output_rows(start):
        at = pl.ds(start, 8)
        mean = means_ref[at]
        live = position8 < mean[:, 7:8]
        kinetic = 0.0
        radial = 0.0
        for k in range(3):
            distance = pos[k, at] - mean[:, k:k + 1]
            radial = radial + distance * distance
            offset = vel[k, at] - mean[:, 3 + k:4 + k]
            kinetic = kinetic + offset * offset
        kin[at] = jnp.where(live, kinetic * mean[:, 6:7], 0.0)
        rad[at] = jnp.where(live, radial, 0.0)

    for c in range(CHUNKS):

        def step(i, carry, c=c):
            output_rows(pl.multiple_of(c * rows + i * 8, 8))
            return carry

        lax.fori_loop(0, rows // 8, step, 0, unroll=True)
        part = pl.ds(c * rows, rows)
        group = [
            pltpu.make_async_copy(kin.at[part], kin_hbm.at[part], sem.at[2 * c]),
            pltpu.make_async_copy(rad.at[part], rad_hbm.at[part], sem.at[2 * c + 1]),
        ]
        for copy in group:
            copy.start()
        stores += group
    for copy in stores:
        copy.wait()


def solution(mesh):
    groups, domains = mesh.shape["grp"], mesh.shape["dom"]

    def local(
        positions, velocities, masses, block_halo, block_shift, block_live, block_count, home_slot
    ):
        blocks, width = masses.shape
        halos = home_slot.shape[0]
        owned = halos // (groups * domains)
        vmem = pl.BlockSpec(memory_space=pltpu.VMEM)
        hbm = pl.BlockSpec(memory_space=pl.ANY)
        dma = pltpu.SemaphoreType.DMA
        pos, vel, means, sums = pl.pallas_call(
            functools.partial(exchange_kernel, groups, domains, owned),
            out_shape=(
                pltpu.VMEM((3, blocks, width), F32),
                pltpu.VMEM((3, blocks, width), F32),
                pltpu.VMEM((blocks, LANES), F32),
                pltpu.VMEM((16, owned), F32),
            ),
            in_specs=[hbm, hbm, hbm, hbm, hbm, hbm, vmem, hbm],
            out_specs=(vmem, vmem, vmem, vmem),
            scratch_shapes=[
                pltpu.VMEM((1, blocks), jnp.int32),
                pltpu.VMEM((3, blocks), jnp.int32),
                pltpu.VMEM((1, blocks), jnp.int32),
                pltpu.VMEM((halos // LANES, LANES), jnp.int32),
                dma((4,)),
                pltpu.VMEM((blocks, width), F32),
                pltpu.VMEM((blocks, LANES), F32),
                pltpu.VMEM((blocks, LANES), F32),
                pltpu.VMEM((domains, 4, 8, owned), F32),
                pltpu.VMEM((domains, 4, 8, owned), F32),
                pltpu.VMEM((2, 8, owned), F32),
                pltpu.VMEM((8, owned), F32),
                pltpu.VMEM((1, 1, owned), F32),
                pltpu.VMEM((domains, 2, 8, owned), F32),
                pltpu.VMEM((domains, 8, owned), F32),
                pltpu.VMEM((domains, 8, owned), F32),
                pltpu.VMEM((8, owned), F32),
                pltpu.VMEM((groups, 1, owned), F32),
                dma((3 * CHUNKS,)),
                dma((domains,)), dma((domains,)),
                dma((domains,)), dma((domains,)),
                dma((domains,)), dma((domains,)),
                dma((domains,)), dma((domains,)),
                dma((domains,)), dma((domains,)),
                dma, dma,
                dma((groups,)), dma((groups,)),
            ],
            compiler_params=pltpu.CompilerParams(collective_id=0, has_side_effects=True),
        )(
            positions, velocities, masses,
            block_halo.reshape(1, blocks), block_shift, block_live.reshape(1, blocks),
            block_count.reshape(1, 1), home_slot.reshape(halos // LANES, LANES),
        )
        return pl.pallas_call(
            functools.partial(output_kernel, halos),
            out_shape=(
                jax.ShapeDtypeStruct((11, owned), F32),
                jax.ShapeDtypeStruct((blocks, width), F32),
                jax.ShapeDtypeStruct((blocks, width), F32),
            ),
            in_specs=[vmem, vmem, vmem, vmem],
            out_specs=(hbm, hbm, hbm),
            scratch_shapes=[
                pltpu.VMEM((11, owned), F32),
                pltpu.VMEM((blocks, width), F32),
                pltpu.VMEM((blocks, width), F32),
                dma((2 * CHUNKS + 1,)),
            ],
        )(*[pltpu.with_memory_space_constraint(x, pltpu.VMEM) for x in (pos, vel, means, sums)])

    return jax.shard_map(
        local,
        mesh=mesh,
        in_specs=(
            P(None, ("grp", "dom"), None),
            P(None, ("grp", "dom"), None),
            P(("grp", "dom"), None),
            P(("grp", "dom")),
            P(None, ("grp", "dom")),
            P(("grp", "dom")),
            P(("grp", "dom")),
            P(),
        ),
        out_specs=(P(None, ("grp", "dom")), P(("grp", "dom"), None), P(("grp", "dom"), None)),
        check_vma=False,
    )
```
